32 devices in a mesh: rep: 2 (over z, core), dp: 16 (over x, y).
Axes of the slice: x: 4, y: 4, z: 1, core: 2. Of those that a mesh axis runs over, the one named last changes fastest.
The devices are a block of a 4x4x8 slice.
Arguments:
- x: bfloat16 [32, 1024, 512], P(('rep', 'dp')), parts along dimension 0
- dy: bfloat16 [32, 1024, 512], P(('rep', 'dp')), parts along dimension 0
- w_gate: bfloat16 [2, 512, 8192], P(None, 'dp')
- w_up: bfloat16 [2, 512, 8192], P(None, 'dp')
- w_down: bfloat16 [2, 8192, 512], P(None, 'dp')
- m_w_gate: float32 [2, 512, 8192], P(None, 'dp')
- m_w_up: float32 [2, 512, 8192], P(None, 'dp')
- m_w_down: float32 [2, 8192, 512], P(None, 'dp')
- v_w_gate: float32 [2, 512, 8192], P(None, 'dp')
- v_w_up: float32 [2, 512, 8192], P(None, 'dp')
- v_w_down: float32 [2, 8192, 512], P(None, 'dp')
Outputs:
- output 1: bfloat16 [4, 512, 8192], P('rep', 'dp'), parts along dimension 0
- output 2: bfloat16 [4, 512, 8192], P('rep', 'dp'), parts along dimension 0
- output 3: bfloat16 [4, 8192, 512], P('rep', 'dp'), parts along dimension 0
- output 4: float32 [4, 512, 8192], P('rep', 'dp'), parts along dimension 0
- output 5: float32 [4, 512, 8192], P('rep', 'dp'), parts along dimension 0
- output 6: float32 [4, 8192, 512], P('rep', 'dp'), parts along dimension 0
- output 7: float32 [4, 512, 8192], P('rep', 'dp'), parts along dimension 0
- output 8: float32 [4, 512, 8192], P('rep', 'dp'), parts along dimension 0
- output 9: float32 [4, 8192, 512], P('rep', 'dp'), parts along dimension 0
There are 2 independent parts. The reference program is written for one: setup_inputs(seed, part) draws one part's arguments, and reference() takes and returns one part's arrays. A program takes and returns all parts, laid end to end along the dimension named above; an argument that names none is the same for every part.
All inputs are finite; a program needn't handle non-finite values.
Results may differ from the reference program's by a relative error of at most 0.022.
Values are sent between devices in bfloat16 or wider.
A program may use at most 768 MiB of HBM per device.

```python
import jax
import jax.numpy as jnp
from jax import lax

SEQUENCES = 16
TOKENS = 1024
D = 512
FF = 8192
LAYERS = 2
NAMES = ("w_gate", "w_up", "w_down")
SHAPES = {"w_gate": (LAYERS, D, FF), "w_up": (LAYERS, D, FF), "w_down": (LAYERS, FF, D)}


def bump(key, n, height):
    away = (jnp.arange(n, dtype=jnp.int32) - jax.random.randint(key, (), 0, n, jnp.int32)) % n
    return jnp.where(away < n // 8, height, 1.0)


def together(key, own, strength):
    shared = jax.random.normal(key, own.shape[1:], jnp.float32)
    return (own + strength * shared) * lax.rsqrt(1 + strength * strength)


def setup_inputs(seed: int = 0, part: int = 0) -> dict:
    kx, kdy, ka, kb, kz, kf, kh, kl, *keys = jax.random.split(jax.random.key(seed), 8 + 3 * len(NAMES))
    kx, kdy, ka, kb = (jax.random.fold_in(k, part) for k in (kx, kdy, ka, kb))
    kw, km, kv = (keys[i::3] for i in range(3))
    shape = (SEQUENCES, TOKENS, D)
    much_x, much_dy = jax.random.uniform(kz, (2,), jnp.float32, 0.0, 1.0)
    loud = 2.0 ** jax.random.uniform(jax.random.fold_in(kz, 1), (), jnp.float32, -1.0, 2.0)
    layers = 2.0 ** jax.random.uniform(kl, (LAYERS, 1, 1), jnp.float32, -1.0, 1.0)
    x = together(ka, jax.random.normal(kx, shape, jnp.float32), much_x) * bump(kf, D, 4.0)
    dy = together(kb, jax.random.normal(kdy, shape, jnp.float32), much_dy)
    drawn = {"x": x.astype(jnp.bfloat16), "dy": (loud * dy * (SEQUENCES * TOKENS) ** -0.5).astype(jnp.bfloat16)}
    for key, name in zip(kw, NAMES, strict=True):
        w = jax.random.normal(key, SHAPES[name], jnp.float32) * SHAPES[name][1] ** -0.5
        drawn[name] = (w * {"w_gate": 1.0, "w_up": bump(kh, FF, 4.0), "w_down": layers}[name]).astype(jnp.bfloat16)
    for key, name in zip(km, NAMES, strict=True):
        drawn[f"m_{name}"] = 0.1 * jax.random.normal(key, SHAPES[name], jnp.float32)
    for key, name in zip(kv, NAMES, strict=True):
        drawn[f"v_{name}"] = jax.random.uniform(key, SHAPES[name], jnp.float32, 0.005, 0.015)
    return drawn


def matmul(a, w):
    return jnp.dot(a, w, preferred_element_type=jnp.float32).astype(jnp.bfloat16)


def normed(h):
    wide = h.astype(jnp.float32)
    scale = lax.rsqrt(jnp.mean(wide**2, -1, keepdims=True) + 1e-6)
    return (wide * scale).astype(jnp.bfloat16)


def layer(h, w):
    a = normed(h)
    gate = jnp.dot(a, w["w_gate"], preferred_element_type=jnp.float32)
    up = jnp.dot(a, w["w_up"], preferred_element_type=jnp.float32)
    return h + matmul((jax.nn.silu(gate) * up).astype(jnp.bfloat16), w["w_down"])


def adamw(w, m, v, g):
    m = 0.9 * m + 0.1 * g
    v = 0.95 * v + 0.05 * g * g
    step = m * lax.rsqrt(v + 1e-8) + 0.1 * w
    return (w - 0.02 * step).astype(jnp.bfloat16), m, v


def stack(weights, h):
    return lax.scan(lambda h, w: (layer(h, w), None), h, weights)[0]


def reference(x, dy, w_gate, w_up, w_down, m_w_gate, m_w_up, m_w_down, v_w_gate, v_w_up, v_w_down):
    weights = dict(zip(NAMES, (w_gate, w_up, w_down), strict=True))

    def take(so_far, sequence):
        h, by_y = sequence
        _, back = jax.vjp(lambda w: stack(w, h), weights)
        return jax.tree.map(lambda total, term: total + term.astype(jnp.float32), so_far, back(by_y)[0]), None

    none_yet = {name: jnp.zeros(w.shape, jnp.float32) for name, w in weights.items()}
    by_weights, _ = lax.scan(take, none_yet, (x, dy))
    gradients = [by_weights[name].astype(jnp.bfloat16).astype(jnp.float32) for name in NAMES]
    new = [
        adamw(w.astype(jnp.float32), m, v, g)
        for w, m, v, g in zip((w_gate, w_up, w_down), (m_w_gate, m_w_up, m_w_down), (v_w_gate, v_w_up, v_w_down), gradients, strict=True)
    ]
    return tuple(one[which] for which in range(3) for one in new)
```

```python
import math

import jax
import jax.numpy as jnp
from jax import lax
from jax.experimental import pallas as pl
from jax.experimental.pallas import tpu as pltpu
from jax.sharding import PartitionSpec as P

MESH = pl.DeviceIdType.MESH
BF16, F32 = jnp.bfloat16, jnp.float32
TILE = 512
SUB = 512
SLOTS = 3


def adamw(w, m, v, g):
    m = 0.9 * m + 0.1 * g
    v = 0.95 * v + 0.05 * g * g
    step = m * lax.rsqrt(v + 1e-8) + 0.1 * w
    return (w - 0.02 * step).astype(BF16), m, v


def nn(a, b):
    return lax.dot_general(a, b, (((1,), (0,)), ((), ())), preferred_element_type=F32)


def nt(a, b):
    return lax.dot_general(a, b, (((1,), (1,)), ((), ())), preferred_element_type=F32)


def scale_of(wide):
    return lax.rsqrt(jnp.mean(wide * wide, -1, keepdims=True) + 1e-6)


def make_kernel(n, tokens, dim, rows, wide_cols, deep, layers):
    total = 2 * tokens
    hidden = wide_cols // 2
    chunk = hidden // n
    subs = chunk // SUB
    tiles = total // TILE
    tiles_seq = tokens // TILE
    per_sub = SUB // deep
    last = layers * n

    def kernel(
        x_ref, dy_ref, wg_ref, wu_ref, wd_ref, pgu, pd,
        GU, D, RG, RD, xb, dyb, a0, a1, aT, dT, pacc, precv, actb, dgb, dub, SGU, SD,
        ld_sem, q_loc, q_send, q_recv, ag_send, ag_recv, ex_send, ex_recv, y_send, y_recv, credit, x_send, p_recv, pd_recv,
    ):
        rep, dp = lax.axis_index("rep"), lax.axis_index("dp")
        c, base = rep % 2, (rep // 2) * 2
        x, y = dp // n, dp % n
        role = x % 2
        sib = (base + 1 - c, dp)

        def at(px, py, core=None):
            return (base + (c if core is None else core), px * n + py)

        def hop(axis, sign):
            return at((x + sign) % n, y) if axis == 0 else at(x, (y + sign) % n)

        for l in range(layers):

            @pl.loop(0, n * n)
            def _(d, l=l):
                for m, w in enumerate((wg_ref, wu_ref)):
                    pltpu.make_async_copy(
                        w.at[l, :, pl.ds(pl.multiple_of(d * 2 * deep + c * deep, deep), deep)],
                        GU.at[l, x, y, :, pl.ds(pl.multiple_of((d // n) * 2 * chunk + m * chunk + (d % n) * deep, deep), deep)],
                        ld_sem.at[l, 0],
                    ).start()

            pltpu.make_async_copy(wd_ref.at[l, pl.ds(pl.multiple_of(c * deep, deep), deep), :], D.at[l, x, y], ld_sem.at[l, 1]).start()

        def own_loaded(l):
            pltpu.make_async_copy(GU.at[l, x, y], GU.at[l, x, y], ld_sem.at[l, 0]).wait()
            pltpu.make_async_copy(D.at[l, x, y], D.at[l, x, y], ld_sem.at[l, 1]).wait()

        barrier = pltpu.get_barrier_semaphore()
        friends = [sib, hop(1, 1), hop(1, -1)]
        for o in range(1, n):
            for core in range(2):
                friends.append(at((x + o) % n, y, core))
        for f in friends:
            pl.semaphore_signal(barrier, inc=1, device_id=f, device_id_type=MESH)
        pl.semaphore_wait(barrier, len(friends))

        def remote(src, dst, ss, rs, dev):
            return pltpu.make_async_remote_copy(src_ref=src, dst_ref=dst, send_sem=ss, recv_sem=rs, device_id=dev, device_id_type=MESH)

        def piece(b, l, path, p, q, half):
            px, py = (p, q) if path == 0 else (q, p)
            if b == 0:
                r, h = rows // 2, wide_cols // 2
                cols = slice(None) if half is None else pl.ds(half * h, h)
                return GU.at[l, px, py, pl.ds(path * r, r), cols]
            r = deep // 2
            if half is None:
                return D.at[l, px, py, pl.ds(path * r, r), :]
            return D.at[l, px, py, pl.ds(path * r + half * (r // 2), r // 2), :]

        def moved(l, path, p, q, half, axis, sign, cls, ev):
            dev = hop(axis if path == 0 else 1 - axis, sign)
            return [
                remote(piece(b, l, path, p, q, half), piece(b, l, path, p, q, half), ag_send.at[l, cls, b], ag_recv.at[l, path, ev, b], dev)
                for b in range(2)
            ]

        def send(*args):
            for one in moved(*args):
                one.start()

        def arrived(l, path, p, q, half, ev):
            for one in moved(l, path, p, q, half, 0, 1, 0, ev):
                one.wait_recv()

        paths = ((0, x, y), (1, y, x))

        def gather(l, stage):
            for path, p, q in paths:
                pm, pp, p2, qm, qp = (p + n - 1) % n, (p + 1) % n, (p + 2) % n, (q + n - 1) % n, (q + 1) % n
                if stage == 0:
                    send(l, path, p, q, None, 0, 1, 0, 0)
                    send(l, path, p, q, None, 0, -1, 0, 1)
                    send(l, path, p, q, None, 1, 1, 0, 4)
                    send(l, path, p, q, None, 1, -1, 0, 9)
                if stage == 1:
                    arrived(l, path, pm, q, None, 0)
                    send(l, path, pm, q, 0, 0, 1, 2, 2)
                    send(l, path, pm, q, None, 1, 1, 0, 5)
                    send(l, path, pm, q, None, 1, -1, 0, 10)
                    arrived(l, path, pp, q, None, 1)
                    send(l, path, pp, q, 1, 0, -1, 2, 3)
                    send(l, path, pp, q, None, 1, 1, 0, 6)
                    send(l, path, pp, q, None, 1, -1, 0, 11)
                if stage == 2:
                    arrived(l, path, p, qm, None, 4)
                    send(l, path, p, qm, 0, 1, 1, 3, 14)
                    arrived(l, path, p, qp, None, 9)
                    send(l, path, p, qp, 1, 1, -1, 3, 14)
                    arrived(l, path, p2, q, 0, 2)
                    send(l, path, p2, q, 0, 1, 1, 1, 7)
                    send(l, path, p2, q, 0, 1, -1, 1, 12)
                    arrived(l, path, p2, q, 1, 3)
                    send(l, path, p2, q, 1, 1, 1, 1, 8)
                    send(l, path, p2, q, 1, 1, -1, 1, 13)
                if stage == 3:
                    arrived(l, path, pm, qm, None, 5)
                    send(l, path, pm, qm, 0, 1, 1, 3, 14)
                    arrived(l, path, pm, qp, None, 10)
                    send(l, path, pm, qp, 1, 1, -1, 3, 14)
                    arrived(l, path, pp, qm, None, 6)
                    send(l, path, pp, qm, 0, 1, 1, 3, 14)
                    arrived(l, path, pp, qp, None, 11)
                    send(l, path, pp, qp, 1, 1, -1, 3, 14)
                if stage == 4:
                    arrived(l, path, p2, qm, 0, 7)
                    send(l, path, p2, qm, 0, 1, 1, 3, 14)
                    arrived(l, path, p2, qp, 1, 13)
                    send(l, path, p2, qp, 1, 1, -1, 3, 14)
                    arrived(l, path, p2, qm, 1, 8)
                    arrived(l, path, p2, qp, 0, 12)
                if stage == 5:
                    for b, W in enumerate((GU, D)):
                        part = W.at[l, 0, pl.ds(0, 2)]
                        remote(part, part, ag_send.at[l, 0, b], ag_recv.at[l, path, 14, b], sib).wait_recv()
            if stage == 5:
                for b, W in enumerate((GU, D)):
                    for cls, part in enumerate((W.at[l, pl.ds(0, 2)], W.at[l, 0, pl.ds(0, 2)], W.at[l, 0, 0], W.at[l, 0])):
                        remote(part, part, ag_send.at[l, cls, b], ag_recv.at[l, 0, 0, b], sib).wait_send()

        primary = c == role
        inputs = ((x_ref, xb), (dy_ref, dyb))

        def to_pair(w):
            src, buf = inputs[w]
            return remote(src.at[0], buf.at[role], q_send.at[w, 0], q_recv.at[w, 1], at(x + 1 - 2 * role, y))

        def to_sib(w, which):
            buf = inputs[w][1]
            slot = role if which == 0 else 1 - role
            return remote(buf.at[slot], buf.at[slot], q_send.at[w, which], q_recv.at[w, which], sib)

        def local(w):
            src, buf = inputs[w]
            return pltpu.make_async_copy(src.at[0], buf.at[role], q_loc.at[w])

        @pl.when(primary)
        def _():
            local(0).start()
            local(1).start()

        own_loaded(0)
        gather(0, 0)

        @pl.when(jnp.logical_not(primary))
        def _():
            to_pair(0).start()

        @pl.when(primary)
        def _():
            for w in range(2):
                local(w).wait()
                to_sib(w, 0).start()

        gather(0, 1)
        gather(0, 2)

        @pl.when(primary)
        def _():
            to_sib(0, 1).wait_recv()
            to_sib(0, 1).start()

        gather(0, 3)
        gather(0, 4)
        own_loaded(1)
        gather(1, 0)

        @pl.when(jnp.logical_not(primary))
        def _():
            to_pair(1).start()
            for which in range(2):
                to_sib(0, which).wait_recv()

        @pl.when(primary)
        def _():
            to_sib(0, 0).wait_send()
            to_sib(0, 1).wait_send()

        def norm(h, a):
            @pl.loop(0, tiles)
            def _(t):
                s, r = t // tiles_seq, pl.ds(pl.multiple_of((t % tiles_seq) * TILE, TILE), TILE)
                wide = h[s, r, :].astype(F32)
                a[pl.ds(pl.multiple_of(t * TILE, TILE), TILE), :] = (wide * scale_of(wide)).astype(BF16)

        def turned(src, dst):
            @pl.loop(0, tiles)
            def _(t):
                dst[:, pl.ds(pl.multiple_of(t * TILE, TILE), TILE)] = src(t).astype(F32).T.astype(BF16)

        def span(t):
            return pl.ds(pl.multiple_of(t * TILE, TILE), TILE)

        def seq_tile(b, t):
            return b[t // tiles_seq, pl.ds(pl.multiple_of((t % tiles_seq) * TILE, TILE), TILE), :]

        norm(xb, a0)

        def clear():
            @pl.loop(0, tiles)
            def _(t):
                pacc[span(t), :] = jnp.zeros((TILE, dim), F32)

        clear()
        gather(0, 5)

        def w_gate(l, j, i):
            return GU.at[l, :, :, :, pl.ds(pl.multiple_of(j * 2 * chunk + i * SUB, SUB), SUB)]

        def w_up(l, j, i):
            return GU.at[l, :, :, :, pl.ds(pl.multiple_of(j * 2 * chunk + chunk + i * SUB, SUB), SUB)]

        def w_down(l, j, i):
            return D.at[l, j, pl.ds(i * per_sub, per_sub), :, :]

        def flat(ref):
            v = ref[...]
            return v.reshape(math.prod(v.shape[:-1]), v.shape[-1])

        def swap_partial():
            part = pacc.at[pl.ds(pl.multiple_of((1 - c) * tokens, tokens), tokens), :]
            return remote(part, precv, ex_send.at[0], ex_recv.at[0], sib)

        def swap_state(buf, which):
            return remote(buf.at[c], buf.at[c], ex_send.at[which], ex_recv.at[which], sib)

        @pl.loop(0, tiles)
        def _(t0):
            t = (t0 + (1 - c) * tiles_seq) % tiles

            @pl.loop(0, n * subs)
            def _(f):
                j, i = f // subs, f % subs
                a = a0[span(t), :]
                gate = nn(a, flat(w_gate(0, j, i)))
                up = nn(a, flat(w_up(0, j, i)))
                act = (gate * jax.nn.sigmoid(gate) * up).astype(BF16)
                pacc[span(t), :] += nn(act, flat(w_down(0, j, i)))

            @pl.when(t0 == tiles_seq - 1)
            def _():
                swap_partial().start()

            for stage in range(1, 5):

                @pl.when(t0 == (stage - 1) * tiles // 4)
                def _(stage=stage):
                    gather(1, stage)

        @pl.when(primary)
        def _():
            to_sib(1, 1).wait_recv()
            to_sib(1, 1).start()

        swap_partial().wait()

        @pl.loop(0, tiles_seq)
        def _(t):
            mine = pl.ds(pl.multiple_of(c * tokens + t * TILE, TILE), TILE)
            out = (pacc[mine, :] + precv[span(t), :]).astype(BF16)
            xb[c, span(t), :] = (xb[c, span(t), :].astype(F32) + out.astype(F32)).astype(BF16)

        swap_state(xb, 1).start()

        @pl.when(primary)
        def _():
            to_sib(1, 0).wait_send()
            to_sib(1, 1).wait_send()

        @pl.when(jnp.logical_not(primary))
        def _():
            for which in range(2):
                to_sib(1, which).wait_recv()
                to_pair(which).wait_send()

        turned(lambda t: seq_tile(dyb, t), dT)
        clear()
        swap_state(xb, 1).wait_send()
        remote(xb.at[1 - c], xb.at[1 - c], ex_send.at[1], ex_recv.at[1], sib).wait_recv()
        norm(xb, a1)
        turned(lambda t: a1[span(t), :], aT)
        gather(1, 5)

        def backward(l, j, a_all, with_da):
            @pl.loop(0, subs)
            def _(i):
                @pl.loop(0, tiles)
                def _(t):
                    a = a_all[span(t), :]
                    wg, wu, wd = flat(w_gate(l, j, i)), flat(w_up(l, j, i)), flat(w_down(l, j, i))
                    gate, up = nn(a, wg), nn(a, wu)
                    dact = nt(seq_tile(dyb, t), wd).astype(BF16).astype(F32)
                    sig = jax.nn.sigmoid(gate)
                    silu = gate * sig
                    actb[span(t), :] = (silu * up).astype(BF16)
                    du = (dact * silu).astype(BF16)
                    dg = (dact * up * (sig + silu * (1.0 - sig))).astype(BF16)
                    dub[span(t), :] = du
                    dgb[span(t), :] = dg
                    if with_da:
                        pacc[span(t), :] += nt(dg, wg) + nt(du, wu)

                shape = (n, n, rows, SUB)
                w_gate(l, j, i)[...] = nn(aT[...], dgb[...]).astype(BF16).reshape(shape)
                w_up(l, j, i)[...] = nn(aT[...], dub[...]).astype(BF16).reshape(shape)
                w_down(l, j, i)[...] = nn(dT[...], actb[...]).T.astype(BF16).reshape(per_sub, deep, dim)

        def where(k):
            return 1 - k // n, (x + k) % n, k % SLOTS

        half_cols, half_rows = chunk, deep // 2

        def own(b, l, j, block, half):
            if b == 0:
                return GU.at[l, :, block, :, pl.ds(pl.multiple_of(j * 2 * chunk + half * chunk, chunk), chunk)]
            return D.at[l, j, block, pl.ds(half * half_rows, half_rows), :]

        ym, yp, y2 = (y + n - 1) % n, (y + 1) % n, (y + 2) % n
        slots = (RG, RD)

        def y_copy(b, src, s, way, kind):
            dst = slots[b].at[s, way, kind]
            return remote(src, dst, y_send.at[s, way, kind, b], y_recv.at[s, way, kind, b], hop(1, -1 if way == 0 else 1))

        def raw(k):
            l, j, s = where(k)
            for way, (near, half_far, half_near) in enumerate(((ym, 0, 1), (yp, 1, 0))):
                for b in range(2):
                    yield y_copy(b, own(b, l, j, y2, half_far), s, way, 0)
                    yield y_copy(b, own(b, l, j, near, half_near), s, way, 1)

        def onward(k):
            l, j, s = where(k)
            for way in range(2):
                for b in range(2):
                    yield y_copy(b, slots[b].at[s, way, 0], s, way, 2)

        def step1(k):
            @pl.when(k >= SLOTS)
            def _():
                pl.semaphore_wait(credit.at[0], 1)
                pl.semaphore_wait(credit.at[1], 1)

            for one in raw(k):
                one.start()

        def step2(k):
            l, j, s = where(k)
            for way, (near, half) in enumerate(((ym, 0), (yp, 1))):
                for b in range(2):
                    slot = slots[b].at[s, way, 0]
                    y_copy(b, slot, s, way, 0).wait_recv()
                    slot[...] = (slot[...].astype(F32) + own(b, l, j, near, half)[...].astype(F32)).astype(BF16)
            for one in onward(k):
                one.start()

        src_id = x // 2

        def outs(k, o):
            l, j, _ = where(k)
            st = k % 2
            there = (x + o) % n
            cols = pl.ds(pl.multiple_of(j * 2 * chunk, 2 * chunk), 2 * chunk)
            return (SGU.at[st, there], pgu.at[src_id, c, l, :, cols], x_send.at[st, o], p_recv.at[src_id, c], at(there, y, role))

        def outs_d(k, o):
            l, j, _ = where(k)
            st = k % 2
            return (SD.at[st], pd.at[src_id, c, l], x_send.at[st, n], pd_recv.at[src_id, c], at((x + o) % n, y, role))

        def each_out(k, act_remote, act_local):
            for o in range(n):
                if o == 0:

                    @pl.when(primary)
                    def _():
                        act_local(pltpu.make_async_copy(*outs(k, 0)[:3]))

                        @pl.when(k % n == 0)
                        def _():
                            act_local(pltpu.make_async_copy(*outs_d(k, 0)[:3]))

                    @pl.when(jnp.logical_not(primary))
                    def _():
                        act_remote(remote(*outs(k, 0)))

                        @pl.when(k % n == 0)
                        def _():
                            act_remote(remote(*outs_d(k, 0)))

                else:
                    act_remote(remote(*outs(k, o)))

                    @pl.when(k % n == o)
                    def _():
                        act_remote(remote(*outs_d(k, o)))

        def outs_done(k):
            each_out(k, lambda d: d.wait_send(), lambda d: d.wait())

        def step3(k):
            l, j, s = where(k)
            st = k % 2
            for way in range(2):
                for b in range(2):
                    for kind in (1, 2):
                        y_copy(b, slots[b].at[s, way, 0], s, way, kind).wait_recv()

            @pl.when(k >= 2)
            def _():
                outs_done(k - 2)

            for half in range(2):
                via, direct = half, 1 - half
                summed = own(0, l, j, y, half)[...].astype(F32) + RG[s, via, 2].astype(F32) + RG[s, direct, 1].astype(F32)
                SGU[st, :, :, pl.ds(half * chunk, chunk)] = summed
                summed = own(1, l, j, y, half)[...].astype(F32) + RD[s, via, 2].astype(F32) + RD[s, direct, 1].astype(F32)
                SD[st, pl.ds(half * half_rows, half_rows), :] = summed
            each_out(k, lambda d: d.start(), lambda d: d.start())
            for one in (*raw(k), *onward(k)):
                one.wait_send()

            @pl.when(k + SLOTS < last)
            def _():
                pl.semaphore_signal(credit.at[1], inc=1, device_id=hop(1, 1), device_id_type=MESH)
                pl.semaphore_signal(credit.at[0], inc=1, device_id=hop(1, -1), device_id_type=MESH)

        @pl.loop(0, last + 2)
        def _(k):
            @pl.when(k < n)
            def _():
                backward(1, (x + k) % n, a1, True)

            @pl.when(k == n)
            def _():
                swap_partial().start()
                turned(lambda t: a0[span(t), :], aT)
                swap_partial().wait()

                @pl.loop(0, tiles_seq)
                def _(t):
                    mine = pl.ds(pl.multiple_of(c * tokens + t * TILE, TILE), TILE)
                    da = (pacc[mine, :] + precv[span(t), :]).astype(BF16).astype(F32)
                    wide = xb[c, span(t), :].astype(F32)
                    scale = scale_of(wide)
                    dh = da * scale - wide * (scale * scale * scale * jnp.mean(da * wide, -1, keepdims=True))
                    dyb[c, span(t), :] = (dyb[c, span(t), :].astype(F32) + dh.astype(BF16).astype(F32)).astype(BF16)

                swap_state(dyb, 2).start()
                swap_state(dyb, 2).wait_send()
                remote(dyb.at[1 - c], dyb.at[1 - c], ex_send.at[2], ex_recv.at[2], sib).wait_recv()
                turned(lambda t: seq_tile(dyb, t), dT)

            @pl.when(jnp.logical_and(k >= n, k < last))
            def _():
                backward(0, (x + k) % n, a0, False)

            @pl.when(k < last)
            def _():
                step1(k)

            @pl.when(jnp.logical_and(k >= 1, k <= last))
            def _():
                step2(k - 1)

            @pl.when(k >= 2)
            def _():
                step3(k - 2)

        outs_done(last - 2)
        outs_done(last - 1)
        for src in range(2):
            for core in range(2):

                @pl.when(jnp.logical_not(jnp.logical_and(primary, jnp.logical_and(src_id == src, c == core))))
                def _(src=src, core=core):
                    remote(pgu.at[src, core], pgu.at[src, core], x_send.at[0, 0], p_recv.at[src, core], sib).wait_recv()
                    remote(pd.at[src, core], pd.at[src, core], x_send.at[0, 0], pd_recv.at[src, core], sib).wait_recv()

    return kernel


def solution(mesh):
    n = math.isqrt(mesh.shape["dp"])

    def partial_sums(x, dy, w_gate, w_up, w_down):
        tokens, dim = x.shape[1:]
        layers, rows, hidden = w_gate.shape
        deep = w_down.shape[1] // 2
        cols = hidden
        chunk = hidden // 2 // n
        total = 2 * tokens
        dma = pltpu.SemaphoreType.DMA
        scratch = [
            pltpu.VMEM((layers, n, n, rows, cols), BF16),
            pltpu.VMEM((layers, n, n, deep, dim), BF16),
            pltpu.VMEM((SLOTS, 2, 3, n, rows, chunk), BF16),
            pltpu.VMEM((SLOTS, 2, 3, deep // 2, dim), BF16),
            pltpu.VMEM((2, tokens, dim), BF16),
            pltpu.VMEM((2, tokens, dim), BF16),
            pltpu.VMEM((total, dim), BF16),
            pltpu.VMEM((total, dim), BF16),
            pltpu.VMEM((dim, total), BF16),
            pltpu.VMEM((dim, total), BF16),
            pltpu.VMEM((total, dim), F32),
            pltpu.VMEM((tokens, dim), F32),
            pltpu.VMEM((total, SUB), BF16),
            pltpu.VMEM((total, SUB), BF16),
            pltpu.VMEM((total, SUB), BF16),
            pltpu.VMEM((2, n, rows, 2 * chunk), F32),
            pltpu.VMEM((2, deep, dim), F32),
            dma((layers, 2)),
            dma((2,)),
            dma((2, 2)),
            dma((2, 2)),
            dma((layers, 4, 2)),
            dma((layers, 2, 15, 2)),
            dma((3,)),
            dma((3,)),
            dma((SLOTS, 2, 3, 2)),
            dma((SLOTS, 2, 3, 2)),
            pltpu.SemaphoreType.REGULAR((2,)),
            dma((2, n + 1)),
            dma((2, 2)),
            dma((2, 2)),
        ]
        return pl.pallas_call(
            make_kernel(n, tokens, dim, rows, cols, deep, layers),
            out_shape=(
                jax.ShapeDtypeStruct((2, 2, layers, rows, cols), F32),
                jax.ShapeDtypeStruct((2, 2, layers, deep, dim), F32),
            ),
            in_specs=[pl.BlockSpec(memory_space=pl.ANY)] * 5,
            out_specs=(pl.BlockSpec(memory_space=pl.ANY),) * 2,
            scratch_shapes=scratch,
            compiler_params=pltpu.CompilerParams(collective_id=0, has_side_effects=True, vmem_limit_bytes=67043328),
        )(x, dy, w_gate, w_up, w_down)

    def step(x, dy, *arrays):
        weights, m, v = (arrays[i : i + 3] for i in (0, 3, 6))
        layers, rows, hidden = weights[0].shape
        deep, dim = weights[2].shape[1] // 2, weights[2].shape[2]
        wide, down = partial_sums(x, dy, *weights)
        wide = wide.sum(0).reshape(2, layers, rows, n, 2, n, deep)
        wide = wide.transpose(4, 1, 2, 3, 5, 0, 6).reshape(2, layers, rows, hidden)
        down = down.sum(0).transpose(1, 0, 2, 3).reshape(layers, 2 * deep, dim)
        gradients = [g.astype(BF16).astype(F32) for g in (wide[0], wide[1], down)]
        new = [adamw(w.astype(F32), m, v, g) for w, m, v, g in zip(weights, m, v, gradients, strict=True)]
        return tuple(one[which] for which in range(3) for one in new)

    states, cut = P(("rep", "dp"), None, None), P(None, "dp", None)
    return jax.shard_map(
        step,
        mesh=mesh,
        in_specs=(states, states) + (cut,) * 9,
        out_specs=(P("rep", "dp", None),) * 9,
        check_vma=False,
    )
```

```python
import math

import jax
import jax.numpy as jnp
from jax import lax
from jax.experimental import pallas as pl
from jax.experimental.pallas import tpu as pltpu
from jax.sharding import PartitionSpec as P

MESH = pl.DeviceIdType.MESH
BF16, F32 = jnp.bfloat16, jnp.float32
TILE = 512
SLOTS = 3


def adamw(w, m, v, g):
    m = 0.9 * m + 0.1 * g
    v = 0.95 * v + 0.05 * g * g
    step = m * lax.rsqrt(v + 1e-8) + 0.1 * w
    return (w - 0.02 * step).astype(BF16), m, v


def nn(a, b):
    return lax.dot_general(a, b, (((1,), (0,)), ((), ())), preferred_element_type=F32)


def nt(a, b):
    return lax.dot_general(a, b, (((1,), (1,)), ((), ())), preferred_element_type=F32)


def sigmoid(a):
    return 0.5 * jnp.tanh(0.5 * a) + 0.5


def scale_of(wide):
    return lax.rsqrt(jnp.mean(wide * wide, -1, keepdims=True) + 1e-6)


def make_kernel(n, tokens, dim, rows, wide_cols, deep, layers):
    total = 2 * tokens
    part = deep // 2
    sub = n * part
    wide = wide_cols // 2
    subs = n // 2
    span_cols = 2 * sub * subs
    chunk = span_cols // 2
    tiles = total // TILE
    tiles_seq = tokens // TILE
    last = layers * n

    def kernel(
        x_ref, dy_ref, wg_ref, wu_ref, wd_ref, far_g, near_g, far_d, near_d,
        GU, D, RG, RD, RX, xb, dyb, a0, a1, aT, dT, pacc, precv, actb, dgb, dub, SB, S32, SDB, SD32,
        ld_sem, q_loc, q_send, q_recv, ag_send, ag_recv, ex_send, ex_recv, y_send, y_recv, m_send, m_recv, credit, x_send, xd_send, p_recv, pd_recv,
    ):
        rep, dp = lax.axis_index("rep"), lax.axis_index("dp")
        c, base = rep % 2, (rep // 2) * 2
        x, y = dp // n, dp % n
        role = x // (n // 2)
        pair, mate = n - 1 - x, x + 1 - 2 * (x % 2)
        sib = (base + 1 - c, dp)

        def at(px, py, core=None):
            return (base + (c if core is None else core), px * n + py)

        def hop(axis, sign):
            return at((x + sign) % n, y) if axis == 0 else at(x, (y + sign) % n)

        for l in range(layers):

            @pl.loop(0, n * n)
            def _(d, l=l):
                for m, w in enumerate((wg_ref, wu_ref)):
                    for h in range(2):
                        to = h * wide + (d // n) * 2 * sub + m * sub + (d % n) * part
                        pltpu.make_async_copy(
                            w.at[l, :, pl.ds(pl.multiple_of(d * 2 * deep + c * deep + h * part, part), part)],
                            GU.at[l, x, y, :, pl.ds(pl.multiple_of(to, part), part)],
                            ld_sem.at[l, 0],
                        ).start()

            for h in range(2):
                rows_h = pl.ds(pl.multiple_of(c * deep + h * part, part), part)
                pltpu.make_async_copy(wd_ref.at[l, rows_h, :], D.at[l, h, x, y], ld_sem.at[l, 1]).start()

        def own_loaded(l):
            pltpu.make_async_copy(GU.at[l, x, y], GU.at[l, x, y], ld_sem.at[l, 0]).wait()
            pltpu.make_async_copy(D.at[l, :, x, y], D.at[l, :, x, y], ld_sem.at[l, 1]).wait()

        barrier = pltpu.get_barrier_semaphore()
        friends = [sib, hop(1, 1), hop(1, -1)]
        for o in range(1, n):
            for core in range(2):
                friends.append(at((x + o) % n, y, core))
        for f in friends:
            pl.semaphore_signal(barrier, inc=1, device_id=f, device_id_type=MESH)
        pl.semaphore_wait(barrier, len(friends))

        def remote(src, dst, ss, rs, dev):
            return pltpu.make_async_remote_copy(src_ref=src, dst_ref=dst, send_sem=ss, recv_sem=rs, device_id=dev, device_id_type=MESH)

        def piece(b, g, path, p, q, half):
            l, h = g // 2, g % 2
            px, py = (p, q) if path == 0 else (q, p)
            if b == 0:
                at_cols = pl.ds(h * wide, wide) if half is None else pl.ds(h * wide + half * (wide // 2), wide // 2)
                return GU.at[l, px, py, pl.ds(path * (rows // 2), rows // 2), at_cols]
            first, count = path * (part // 2), part // 2
            if half is not None:
                first, count = first + half * (count // 2), count // 2
            return D.at[l, h, px, py, pl.ds(first, count), :]

        def blocks(b, g, which):
            if b == 0:
                return GU.at[(g // 2, *which, slice(None), pl.ds((g % 2) * wide, wide))]
            return D.at[(g // 2, g % 2, *which)]

        def moved(l, path, p, q, half, axis, sign, cls, ev):
            dev = hop(axis if path == 0 else 1 - axis, sign)
            return [
                remote(piece(b, l, path, p, q, half), piece(b, l, path, p, q, half), ag_send.at[l, cls, b], ag_recv.at[l, path, ev, b], dev)
                for b in range(2)
            ]

        def send(*args):
            for one in moved(*args):
                one.start()

        def arrived(l, path, p, q, half, ev):
            for one in moved(l, path, p, q, half, 0, 1, 0, ev):
                one.wait_recv()

        paths = ((0, x, y), (1, y, x))

        def spread(g, path, p, q, half, cls, ev):
            send(g, path, p, q, half, 1, 1, cls, ev)
            send(g, path, p, q, half, 1, -1, cls, ev + 5)

        def relay(g, path, p, ends, whole, ev, step):
            for half, sign in enumerate((1, -1)):
                arrived(g, path, p, ends[half], None if whole else half, ev + step * half)
                send(g, path, p, ends[half], half, 1, sign, 3, 14)

        def gather(g, stage):
            for path, p, q in paths:
                sides, across, ends = ((p + n - 1) % n, (p + 1) % n), (p + 2) % n, ((q + n - 1) % n, (q + 1) % n)
                if stage == 0:
                    for half, sign in enumerate((1, -1)):
                        send(g, path, p, q, None, 0, sign, 0, half)
                    spread(g, path, p, q, None, 0, 4)
                if stage == 1:
                    for half, sign in enumerate((1, -1)):
                        arrived(g, path, sides[half], q, None, half)
                        send(g, path, sides[half], q, half, 0, sign, 2, 2 + half)
                        spread(g, path, sides[half], q, None, 0, 5 + half)
                if stage == 2:
                    relay(g, path, p, ends, True, 4, 5)
                    for half in range(2):
                        arrived(g, path, across, q, half, 2 + half)
                        spread(g, path, across, q, half, 1, 7 + half)
                if stage == 3:
                    for half in range(2):
                        relay(g, path, sides[half], ends, True, 5 + half, 5)
                if stage == 4:
                    relay(g, path, across, ends, False, 7, 6)
                    for half in range(2):
                        arrived(g, path, across, ends[half], 1 - half, 8 + 4 * half)
                if stage == 5:
                    for b in range(2):
                        size = blocks(b, g, (0, pl.ds(0, 2)))
                        remote(size, size, ag_send.at[g, 0, b], ag_recv.at[g, path, 14, b], sib).wait_recv()
            if stage == 5:
                every = slice(None)
                for b in range(2):
                    for cls, which in enumerate(((pl.ds(0, 2), every), (0, pl.ds(0, 2)), (0, 0), (0, every))):
                        size = blocks(b, g, which)
                        remote(size, size, ag_send.at[g, cls, b], ag_recv.at[g, 0, 0, b], sib).wait_send()

        primary = c == role
        inputs = ((x_ref, xb), (dy_ref, dyb))

        def to_pair(w):
            src, buf = inputs[w]
            return remote(src.at[0], buf.at[role], q_send.at[w, 0], q_recv.at[w, 1], at(pair, y))

        def to_sib(w, which):
            buf = inputs[w][1]
            slot = role if which == 0 else 1 - role
            return remote(buf.at[slot], buf.at[slot], q_send.at[w, which], q_recv.at[w, which], sib)

        def local(w):
            src, buf = inputs[w]
            return pltpu.make_async_copy(src.at[0], buf.at[role], q_loc.at[w])

        @pl.when(primary)
        def _():
            local(0).start()
            local(1).start()

        own_loaded(0)
        gather(0, 0)

        @pl.when(jnp.logical_not(primary))
        def _():
            to_pair(0).start()

        @pl.when(primary)
        def _():
            for w in range(2):
                local(w).wait()
                to_sib(w, 0).start()

        gather(0, 1)
        gather(0, 2)

        @pl.when(primary)
        def _():
            to_sib(0, 1).wait_recv()
            to_sib(0, 1).start()

        gather(0, 3)
        gather(1, 0)
        gather(0, 4)

        @pl.when(jnp.logical_not(primary))
        def _():
            to_pair(1).start()
            for which in range(2):
                to_sib(0, which).wait_recv()

        @pl.when(primary)
        def _():
            to_sib(0, 0).wait_send()
            to_sib(0, 1).wait_send()

        def norm(h, a):
            @pl.loop(0, tiles)
            def _(t):
                s, r = t // tiles_seq, pl.ds(pl.multiple_of((t % tiles_seq) * TILE, TILE), TILE)
                wide = h[s, r, :].astype(F32)
                a[pl.ds(pl.multiple_of(t * TILE, TILE), TILE), :] = (wide * scale_of(wide)).astype(BF16)

        def turned(src, dst):
            @pl.loop(0, tiles)
            def _(t):
                dst[:, pl.ds(pl.multiple_of(t * TILE, TILE), TILE)] = src(t).astype(F32).T.astype(BF16)

        def span(t):
            return pl.ds(pl.multiple_of(t * TILE, TILE), TILE)

        def seq_tile(b, t):
            return b[t // tiles_seq, pl.ds(pl.multiple_of((t % tiles_seq) * TILE, TILE), TILE), :]

        norm(xb, a0)

        def clear():
            @pl.loop(0, tiles)
            def _(t):
                pacc[span(t), :] = jnp.zeros((TILE, dim), F32)

        clear()
        gather(0, 5)

        def w_gate(l, h, j):
            return GU.at[l, :, :, :, pl.ds(pl.multiple_of(h * wide + j * 2 * sub, sub), sub)]

        def w_up(l, h, j):
            return GU.at[l, :, :, :, pl.ds(pl.multiple_of(h * wide + j * 2 * sub + sub, sub), sub)]

        def w_down(l, h, j):
            return D.at[l, h, j]

        def flat(ref):
            v = ref[...]
            return v.reshape(math.prod(v.shape[:-1]), v.shape[-1])

        def swap_partial():
            part = pacc.at[pl.ds(pl.multiple_of((1 - c) * tokens, tokens), tokens), :]
            return remote(part, precv, ex_send.at[0], ex_recv.at[0], sib)

        def swap_state(buf, which):
            return remote(buf.at[c], buf.at[c], ex_send.at[which], ex_recv.at[which], sib)

        for h in range(2):

            @pl.loop(0, tiles)
            def _(t0, h=h):
                t = (t0 + (1 - c) * tiles_seq) % tiles

                @pl.loop(0, n)
                def _(j):
                    a = a0[span(t), :]
                    gate = nn(a, flat(w_gate(0, h, j)))
                    up = nn(a, flat(w_up(0, h, j)))
                    act = (gate * sigmoid(gate) * up).astype(BF16)
                    pacc[span(t), :] += nn(act, flat(w_down(0, h, j)))

                if h == 1:

                    @pl.when(t0 == tiles_seq - 1)
                    def _():
                        swap_partial().start()

                for stage in range(1, 5):

                    @pl.when(t0 == (stage - 1) * tiles // 4)
                    def _(stage=stage):
                        gather(1 + h, stage)
                        if stage == 3:
                            if h == 0:
                                own_loaded(1)
                            gather(2 + h, 0)

            if h == 0:
                gather(1, 5)

        @pl.when(primary)
        def _():
            to_sib(1, 1).wait_recv()
            to_sib(1, 1).start()

        swap_partial().wait()

        @pl.loop(0, tiles_seq)
        def _(t):
            mine = pl.ds(pl.multiple_of(c * tokens + t * TILE, TILE), TILE)
            out = (pacc[mine, :] + precv[span(t), :]).astype(BF16)
            xb[c, span(t), :] = (xb[c, span(t), :].astype(F32) + out.astype(F32)).astype(BF16)

        swap_state(xb, 1).start()

        @pl.when(primary)
        def _():
            to_sib(1, 0).wait_send()
            to_sib(1, 1).wait_send()

        @pl.when(jnp.logical_not(primary))
        def _():
            for which in range(2):
                to_sib(1, which).wait_recv()
                to_pair(which).wait_send()

        turned(lambda t: seq_tile(dyb, t), dT)
        clear()
        swap_state(xb, 1).wait_send()
        remote(xb.at[1 - c], xb.at[1 - c], ex_send.at[1], ex_recv.at[1], sib).wait_recv()
        norm(xb, a1)
        turned(lambda t: a1[span(t), :], aT)
        gather(2, 5)

        def where(k):
            return 1 - k // n, (k % n) // 2, k % 2, k % SLOTS

        def own(b, k, block, half, px=None):
            l, h, jj, _ = where(k)
            if b == 0:
                cols = pl.ds(pl.multiple_of(h * wide + jj * span_cols + half * chunk, chunk), chunk)
                return GU.at[l, slice(None) if px is None else px, block, :, cols]
            return D.at[l, h, kept_x(k), block, pl.ds(half * (part // 2), part // 2), :]

        def kept_x(k):
            jj = k % 2
            same = 1 - (x // subs + jj) % 2
            return same * x + (1 - same) * pair

        def given_x(k):
            return 2 * subs * (k % 2) + 1 - kept_x(k)

        def to_mate(k):
            l, h, _, s = where(k)
            return remote(D.at[l, h, given_x(k)], RX.at[s], m_send.at[s], m_recv.at[s], at(mate, y))

        def from_mate(k, block, half):
            return RX.at[k % SLOTS, block, pl.ds(half * (part // 2), part // 2), :]

        def backward(l, k, a_all, with_da):
            h = (k % n) // 2

            @pl.loop(0, subs)
            def _(i):
                j = i * kept_x(k) + (1 - i) * given_x(k)

                @pl.loop(0, tiles)
                def _(t):
                    a = a_all[span(t), :]
                    wg, wu, wd = flat(w_gate(l, h, j)), flat(w_up(l, h, j)), flat(w_down(l, h, j))
                    gate, up = nn(a, wg), nn(a, wu)
                    dact = nt(seq_tile(dyb, t), wd).astype(BF16).astype(F32)
                    sig = sigmoid(gate)
                    silu = gate * sig
                    actb[span(t), :] = (silu * up).astype(BF16)
                    du = (dact * silu).astype(BF16)
                    dg = (dact * up * (sig + silu * (1.0 - sig))).astype(BF16)
                    dub[span(t), :] = du
                    dgb[span(t), :] = dg
                    if with_da:
                        pacc[span(t), :] += nt(dg, wg) + nt(du, wu)

                shape = (n, n, rows, sub)
                w_gate(l, h, j)[...] = nn(aT[...], dgb[...]).astype(BF16).reshape(shape)
                w_up(l, h, j)[...] = nn(aT[...], dub[...]).astype(BF16).reshape(shape)
                w_down(l, h, j)[...] = nn(dT[...], actb[...]).T.astype(BF16).reshape(n, part, dim)

                @pl.when(i == 0)
                def _():
                    @pl.when(k >= SLOTS)
                    def _():
                        pl.semaphore_wait(credit.at[2], 1)

                    to_mate(k).start()

                    @pl.when(k >= 1)
                    def _():
                        step2(k - 1)

                if l == 1:
                    for stage in range(1, 5):

                        @pl.when(k * subs + i == stage - 1)
                        def _(stage=stage):
                            gather(3, stage)

        ym, yp, y2 = (y + n - 1) % n, (y + 1) % n, (y + 2) % n
        slots = (RG, RD)

        def y_copy(b, src, s, way, kind):
            dst = slots[b].at[s, way, kind]
            return remote(src, dst, y_send.at[s, way, kind, b], y_recv.at[s, way, kind, b], hop(1, -1 if way == 0 else 1))

        def raw(b, k):
            s = k % SLOTS
            source = own if b == 0 else lambda _, k, block, half: from_mate(k, block, half)
            for way, (near, half_far, half_near) in enumerate(((ym, 0, 1), (yp, 1, 0))):
                yield y_copy(b, source(b, k, y2, half_far), s, way, 0)
                yield y_copy(b, source(b, k, near, half_near), s, way, 1)

        def onward(k):
            s = k % SLOTS
            for way in range(2):
                for b in range(2):
                    yield y_copy(b, slots[b].at[s, way, 0], s, way, 2)

        def step1(k):
            @pl.when(k >= SLOTS)
            def _():
                pl.semaphore_wait(credit.at[0], 1)
                pl.semaphore_wait(credit.at[1], 1)

            for one in raw(0, k):
                one.start()

        def term(b, k, block, half, px=None):
            mine = own(b, k, block, half, px)[...].astype(F32)
            return mine if b == 0 else mine + from_mate(k, block, half)[...].astype(F32)

        def step1_down(k):
            to_mate(k).wait_recv()
            for block, half in ((y2, 0), (y2, 1), (ym, 1), (yp, 0)):
                from_mate(k, block, half)[...] = term(1, k, block, half).astype(BF16)
            for one in raw(1, k):
                one.start()

        def step2(k):
            s = k % SLOTS
            for way, (near, half) in enumerate(((ym, 0), (yp, 1))):
                for b in range(2):
                    slot = slots[b].at[s, way, 0]
                    y_copy(b, slot, s, way, 0).wait_recv()
                    slot[...] = (slot[...].astype(F32) + term(b, k, near, half)).astype(BF16)
            for one in onward(k):
                one.start()

        def near_out(k, src, dst, ss, rs, act_remote, act_local):
            @pl.when(primary)
            def _():
                act_local(pltpu.make_async_copy(src, dst, ss))

            @pl.when(jnp.logical_not(primary))
            def _():
                act_remote(remote(src, dst, ss, rs, sib))

        def each_out(k, act_remote, act_local):
            l, h, jj, _ = where(k)
            st = k % 2
            cols = pl.ds(pl.multiple_of(h * wide + jj * span_cols, span_cols), span_cols)
            near_out(k, S32.at[st], near_g.at[c, l, :, cols], x_send.at[st, 0], p_recv.at[2, c], act_remote, act_local)
            for o in range(1, n):
                there, far = (x + o) % n, int(o == 2)
                act_remote(remote(SB.at[st, there], far_g.at[far, c, l, :, cols], x_send.at[st, o], p_recv.at[far, c], at(there, y, role)))
            at_rows = pl.ds(pl.multiple_of(c * deep + h * part, part), part)
            here = x // subs == jj

            @pl.when(here)
            def _():
                near_out(k, SD32.at[st], near_d.at[l, at_rows], xd_send.at[st], pd_recv.at[1, c], act_remote, act_local)

            @pl.when(jnp.logical_not(here))
            def _():
                act_remote(remote(SDB.at[st], far_d.at[l, at_rows], xd_send.at[st], pd_recv.at[0, c], at(pair, y, role)))

        def outs_done(k):
            each_out(k, lambda d: d.wait_send(), lambda d: d.wait())

        def step3(k):
            s, st = k % SLOTS, k % 2
            for way in range(2):
                for b in range(2):
                    for kind in (1, 2):
                        y_copy(b, slots[b].at[s, way, 0], s, way, kind).wait_recv()

            @pl.when(k >= 2)
            def _():
                outs_done(k - 2)

            for half in range(2):
                via, direct = half, 1 - half
                cols = pl.ds(half * chunk, chunk)
                for px in range(n):
                    summed = own(0, k, y, half, px)[...].astype(F32) + RG[s, via, 2, px].astype(F32) + RG[s, direct, 1, px].astype(F32)
                    SB[st, px, :, cols] = summed.astype(BF16)

                    @pl.when(x == px)
                    def _(summed=summed, cols=cols):
                        S32[st, :, cols] = summed

                summed = term(1, k, y, half) + RD[s, via, 2].astype(F32) + RD[s, direct, 1].astype(F32)
                at_rows = pl.ds(half * (part // 2), part // 2)
                SDB[st, at_rows, :] = summed.astype(BF16)
                SD32[st, at_rows, :] = summed

            each_out(k, lambda d: d.start(), lambda d: d.start())
            for one in (*raw(0, k), *raw(1, k), *onward(k), to_mate(k)):
                one.wait_send()

            @pl.when(k + SLOTS < last)
            def _():
                pl.semaphore_signal(credit.at[1], inc=1, device_id=hop(1, 1), device_id_type=MESH)
                pl.semaphore_signal(credit.at[0], inc=1, device_id=hop(1, -1), device_id_type=MESH)
                pl.semaphore_signal(credit.at[2], inc=1, device_id=at(mate, y), device_id_type=MESH)

        @pl.loop(0, last + 1)
        def _(k):
            @pl.when(k < n)
            def _():
                @pl.when(k == 2)
                def _():
                    gather(3, 5)

                backward(1, k, a1, True)

                @pl.when(k == n - 1)
                def _():
                    swap_partial().start()

            @pl.when(k == n)
            def _():
                turned(lambda t: a0[span(t), :], aT)
                swap_partial().wait()

                @pl.loop(0, tiles_seq)
                def _(t):
                    mine = pl.ds(pl.multiple_of(c * tokens + t * TILE, TILE), TILE)
                    da = (pacc[mine, :] + precv[span(t), :]).astype(BF16).astype(F32)
                    wide = xb[c, span(t), :].astype(F32)
                    scale = scale_of(wide)
                    dh = da * scale - wide * (scale * scale * scale * jnp.mean(da * wide, -1, keepdims=True))
                    dyb[c, span(t), :] = (dyb[c, span(t), :].astype(F32) + dh.astype(BF16).astype(F32)).astype(BF16)

                swap_state(dyb, 2).start()
                swap_state(dyb, 2).wait_send()
                remote(dyb.at[1 - c], dyb.at[1 - c], ex_send.at[2], ex_recv.at[2], sib).wait_recv()
                turned(lambda t: seq_tile(dyb, t), dT)

            @pl.when(jnp.logical_and(k >= n, k < last))
            def _():
                backward(0, k, a0, False)

            @pl.when(k < last)
            def _():
                step1(k)

            @pl.when(k == last)
            def _():
                step2(k - 1)

            @pl.when(k >= 1)
            def _():
                step3(k - 1)

            @pl.when(k < last)
            def _():
                step1_down(k)

        outs_done(last - 2)
        outs_done(last - 1)

        def landed(part_of, sem):
            remote(part_of, part_of, x_send.at[0, 0], sem, sib).wait_recv()

        for core in range(2):
            landed(far_g.at[0, core], p_recv.at[0, core])

            @pl.when(jnp.logical_not(primary))
            def _(core=core):
                landed(far_g.at[1, core], p_recv.at[1, core])
                landed(far_d.at[0], pd_recv.at[0, core])

            @pl.when(jnp.logical_and(primary, c != core))
            def _(core=core):
                landed(near_g.at[core], p_recv.at[2, core])
                landed(near_d.at[0], pd_recv.at[1, core])

    return kernel


def gated_adamw(n, deep):
    part = deep // 2
    sub = n * part

    def kernel(near_ref, far_ref, g_ref, wg, mg, vg, wu, mu, vu, owg, owu, omg, omu, ovg, ovu):
        near = near_ref[0] != 0
        wide = far_ref.shape[-1] // 2
        for i, (w, m, v, ow, om, ov) in enumerate(((wg, mg, vg, owg, omg, ovg), (wu, mu, vu, owu, omu, ovu))):
            for d in range(n * n):
                for core in range(2):
                    for h in range(2):
                        first = h * wide + (d // n) * 2 * sub + i * sub + (d % n) * part
                        cols = slice(first, first + part)
                        other = jnp.where(near, g_ref[core, 0, :, cols], far_ref[1, core, 0, :, cols].astype(F32))
                        g = (far_ref[0, core, 0, :, cols].astype(F32) + other).astype(BF16).astype(F32)
                        first = d * 2 * deep + core * deep + h * part
                        cols = slice(first, first + part)
                        at = (0, slice(None), cols)
                        ow[at], om[at], ov[at] = adamw(w[at].astype(F32), m[at], v[at], g)

    return kernel


def solution(mesh):
    n = math.isqrt(mesh.shape["dp"])

    def partial_sums(x, dy, w_gate, w_up, w_down):
        tokens, dim = x.shape[1:]
        layers, rows, hidden = w_gate.shape
        deep = w_down.shape[1] // 2
        cols = hidden
        chunk = hidden // 2 // n
        part = deep // 2
        sub = n * part
        total = 2 * tokens
        dma = pltpu.SemaphoreType.DMA
        scratch = [
            pltpu.VMEM((layers, n, n, rows, cols), BF16),
            pltpu.VMEM((layers, 2, n, n, part, dim), BF16),
            pltpu.VMEM((SLOTS, 2, 3, n, rows, chunk), BF16),
            pltpu.VMEM((SLOTS, 2, 3, part // 2, dim), BF16),
            pltpu.VMEM((SLOTS, n, part, dim), BF16),
            pltpu.VMEM((2, tokens, dim), BF16),
            pltpu.VMEM((2, tokens, dim), BF16),
            pltpu.VMEM((total, dim), BF16),
            pltpu.VMEM((total, dim), BF16),
            pltpu.VMEM((dim, total), BF16),
            pltpu.VMEM((dim, total), BF16),
            pltpu.VMEM((total, dim), F32),
            pltpu.VMEM((tokens, dim), F32),
            pltpu.VMEM((total, sub), BF16),
            pltpu.VMEM((total, sub), BF16),
            pltpu.VMEM((total, sub), BF16),
            pltpu.VMEM((2, n, rows, 2 * chunk), BF16),
            pltpu.VMEM((2, rows, 2 * chunk), F32),
            pltpu.VMEM((2, part, dim), BF16),
            pltpu.VMEM((2, part, dim), F32),
            dma((layers, 2)),
            dma((2,)),
            dma((2, 2)),
            dma((2, 2)),
            dma((2 * layers, 4, 2)),
            dma((2 * layers, 2, 15, 2)),
            dma((3,)),
            dma((3,)),
            dma((SLOTS, 2, 3, 2)),
            dma((SLOTS, 2, 3, 2)),
            dma((SLOTS,)),
            dma((SLOTS,)),
            pltpu.SemaphoreType.REGULAR((3,)),
            dma((2, n)),
            dma((2,)),
            dma((3, 2)),
            dma((2, 2)),
        ]
        return pl.pallas_call(
            make_kernel(n, tokens, dim, rows, cols, deep, layers),
            out_shape=(
                jax.ShapeDtypeStruct((2, 2, layers, rows, cols), BF16),
                jax.ShapeDtypeStruct((2, layers, rows, cols), F32),
                jax.ShapeDtypeStruct((layers, 2 * deep, dim), BF16),
                jax.ShapeDtypeStruct((layers, 2 * deep, dim), F32),
            ),
            in_specs=[pl.BlockSpec(memory_space=pl.ANY)] * 5,
            out_specs=(pl.BlockSpec(memory_space=pl.ANY),) * 4,
            scratch_shapes=scratch,
            compiler_params=pltpu.CompilerParams(collective_id=0, has_side_effects=True, vmem_limit_bytes=67043328),
        )(x, dy, w_gate, w_up, w_down)

    def step(x, dy, *arrays):
        wg, wu, wd, mg, mu, md, vg, vu, vd = arrays
        layers, rows, hidden = wg.shape
        deep = wd.shape[1] // 2
        far_g, near_g, far_d, near_d = partial_sums(x, dy, wg, wu, wd)
        near = lax.axis_index("rep") % 2 == (lax.axis_index("dp") // n) // (n // 2)
        tall = 16

        def cut_rows(*lead):
            return pl.BlockSpec((*lead, 1, tall, hidden), lambda l, r: (*(0 for _ in lead), l, r, 0))

        like = [jax.ShapeDtypeStruct(one.shape, kind) for kind, one in ((BF16, wg), (F32, mg), (F32, vg)) for _ in range(2)]
        wide = pl.pallas_call(
            gated_adamw(n, deep),
            grid=(layers, rows // tall),
            out_shape=like,
            in_specs=[pl.BlockSpec(memory_space=pltpu.SMEM), cut_rows(2, 2), cut_rows(2)] + [cut_rows()] * 6,
            out_specs=[cut_rows()] * 6,
        )(near.astype(jnp.int32)[None], far_g, near_g, wg, mg, vg, wu, mu, vu)
        g = jnp.where(near, near_d, far_d.astype(F32))
        down = adamw(wd.astype(F32), md, vd, g.astype(BF16).astype(F32))
        pairs = zip(wide[::2], wide[1::2], down, strict=True)
        return tuple(one for three in pairs for one in three)

    states, cut = P(("rep", "dp"), None, None), P(None, "dp", None)
    return jax.shard_map(
        step,
        mesh=mesh,
        in_specs=(states, states) + (cut,) * 9,
        out_specs=(P("rep", "dp", None),) * 9,
        check_vma=False,
    )
```
